16 devices in a mesh: dp: 2 (over y, z), cp: 8 (over x, core).
Axes of the slice: x: 4, y: 2, z: 1, core: 2. Of those that a mesh axis runs over, the one named last changes fastest.
The devices are a block of a 4x4x8 slice.
Arguments:
- hidden: bfloat16 [16384, 2048], P(('dp', 'cp')), parts along dimension 0
- seg_id: int32 [16384], P(('dp', 'cp')), parts along dimension 0
- doc_pos: int32 [16384], P(('dp', 'cp')), parts along dimension 0
- norm_gain: bfloat16 [2048], replicated
- w_qkv: bfloat16 [2048, 2560], replicated
- b_qkv: bfloat16 [2560], replicated
- w_out: bfloat16 [2048, 2048], replicated
- grad_out: bfloat16 [16384, 2048], P(('dp', 'cp')), parts along dimension 0
Outputs:
- output 1: bfloat16 [16384, 2048], P(('dp', 'cp')), parts along dimension 0
- output 2: bfloat16 [16384, 2048], P(('dp', 'cp')), parts along dimension 0
- output 3: float32 [4096], P('dp'), parts along dimension 0
- output 4: float32 [4096, 2560], P('dp'), parts along dimension 0
- output 5: float32 [5120], P('dp'), parts along dimension 0
- output 6: float32 [4096, 2048], P('dp'), parts along dimension 0
There are 2 independent parts. The reference program is written for one: setup_inputs(seed, part) draws one part's arguments, and reference() takes and returns one part's arrays. A program takes and returns all parts, laid end to end along the dimension named above; an argument that names none is the same for every part.
All inputs are finite; a program needn't handle non-finite values.
Results may differ from the reference program's by a relative error of at most 0.0188335.
Values are sent between devices in bfloat16 or wider.
A program may use at most 768 MiB of HBM per device.

```python
import jax
import jax.numpy as jnp
from jax import lax

D = 2048
HEADS = 16
GROUPS = 2
HEAD = 128
SEQ = 8192
DOCS = 4
BLOCK = 128

ROT_DIMS = HEAD // 2
REP_HEADS = HEADS // GROUPS
ATT_WIDTH = HEADS * HEAD
KV_WIDTH = GROUPS * HEAD
QKV_WIDTH = ATT_WIDTH + 2 * KV_WIDTH
ROPE_BASE = 5000000.0
EPS_NORM = 1e-5
NEG_BIG = -1e30


def draw_documents(doc_key):
    cut_points = jax.random.permutation(doc_key, SEQ - 1)[: DOCS - 1] + 1
    start_flag = jnp.zeros((SEQ,), jnp.int32).at[cut_points].set(1)
    seg_id = jnp.cumsum(start_flag).astype(jnp.int32)
    tok_index = jnp.arange(SEQ, dtype=jnp.int32)
    doc_start = lax.cummax(jnp.where(start_flag > 0, tok_index, 0), axis=0)
    return seg_id, (tok_index - doc_start).astype(jnp.int32)


def setup_inputs(seed: int = 0, part: int = 0) -> dict:
    root_key = jax.random.key(seed)
    key_gain, key_wqkv, key_bqkv, key_wout = jax.random.split(root_key, 4)
    part_key = jax.random.fold_in(root_key, part)
    key_x, key_doc, key_dy = jax.random.split(part_key, 3)
    seg_id, doc_pos = draw_documents(key_doc)
    hidden = jax.random.normal(key_x, (SEQ, D), jnp.float32)
    norm_gain = 1.0 + 0.3 * jax.random.normal(key_gain, (D,), jnp.float32)
    w_qkv = 1.5 * D ** -0.5 * jax.random.normal(key_wqkv, (D, QKV_WIDTH), jnp.float32)
    b_qkv = 0.5 * jax.random.normal(key_bqkv, (QKV_WIDTH,), jnp.float32)
    w_out = ATT_WIDTH ** -0.5 * jax.random.normal(key_wout, (ATT_WIDTH, D), jnp.float32)
    grad_out = jax.random.normal(key_dy, (SEQ, D), jnp.float32)
    return {
        'hidden': hidden.astype(jnp.bfloat16),
        'seg_id': seg_id,
        'doc_pos': doc_pos,
        'norm_gain': norm_gain.astype(jnp.bfloat16),
        'w_qkv': w_qkv.astype(jnp.bfloat16),
        'b_qkv': b_qkv.astype(jnp.bfloat16),
        'w_out': w_out.astype(jnp.bfloat16),
        'grad_out': grad_out.astype(jnp.bfloat16),
    }


def rotate(values, cos_ang, sin_ang):
    rot_pairs = values[..., :ROT_DIMS].reshape(values.shape[:-1] + (ROT_DIMS // 2, 2))
    even_part = rot_pairs[..., 0]
    odd_part = rot_pairs[..., 1]
    turned = jnp.stack([even_part * cos_ang - odd_part * sin_ang, odd_part * cos_ang + even_part * sin_ang], axis=-1)
    return jnp.concatenate([turned.reshape(values.shape[:-1] + (ROT_DIMS,)), values[..., ROT_DIMS:]], axis=-1)


def attention_core(q_rot, k_rot, v_val, seg_id):
    n_blocks = SEQ // BLOCK
    scale = HEAD ** -0.5
    q_blocks = q_rot.reshape(n_blocks, BLOCK, GROUPS, REP_HEADS, HEAD)
    k_blocks = k_rot.reshape(n_blocks, BLOCK, GROUPS, HEAD)
    v_blocks = v_val.reshape(n_blocks, BLOCK, GROUPS, HEAD)
    seg_blocks = seg_id.reshape(n_blocks, BLOCK)
    offsets = jnp.arange(BLOCK)

    def query_block(blk_args):
        q_idx, q_blk, seg_q = blk_args

        def key_step(loop_vals, key_args):
            k_idx, k_blk, v_blk, seg_k = key_args
            vis_mask = (seg_q[:, None] == seg_k[None, :]) & (k_idx * BLOCK + offsets[None, :] <= q_idx * BLOCK + offsets[:, None])

            def advance(run_state):
                m_run, l_run, acc_sum = run_state
                scores = jnp.einsum('qgrd,kgd->grqk', q_blk, k_blk) * scale
                scores = jnp.where(vis_mask, scores, NEG_BIG)
                m_new = jnp.maximum(m_run, jnp.max(scores, axis=-1))
                p_mat = jnp.where(vis_mask, jnp.exp(scores - m_new[..., None]), 0.0)
                rescale = jnp.exp(m_run - m_new)
                return (m_new, l_run * rescale + jnp.sum(p_mat, axis=-1), acc_sum * rescale[..., None] + jnp.einsum('grqk,kgd->grqd', p_mat, v_blk))

            return lax.cond(jnp.any(vis_mask), advance, lambda run_state: run_state, loop_vals), None

        init_state = (
            jnp.full((GROUPS, REP_HEADS, BLOCK), NEG_BIG, jnp.float32),
            jnp.zeros((GROUPS, REP_HEADS, BLOCK), jnp.float32),
            jnp.zeros((GROUPS, REP_HEADS, BLOCK, HEAD), jnp.float32),
        )
        final_state, _ = lax.scan(jax.checkpoint(key_step), init_state, (jnp.arange(n_blocks), k_blocks, v_blocks, seg_blocks))
        return final_state[2] / final_state[1][..., None]

    context = lax.map(jax.checkpoint(query_block), (jnp.arange(n_blocks), q_blocks, seg_blocks))
    return context.transpose(0, 3, 1, 2, 4).reshape(SEQ, GROUPS, REP_HEADS, HEAD)


def reference(hidden, seg_id, doc_pos, norm_gain, w_qkv, b_qkv, w_out, grad_out):
    hid_f32 = hidden.astype(jnp.float32)
    inv_rms = lax.rsqrt(jnp.mean(hid_f32 * hid_f32, axis=-1, keepdims=True) + EPS_NORM)
    x_hat = hid_f32 * inv_rms
    gain_f32 = norm_gain.astype(jnp.float32)
    normed = (x_hat * gain_f32).astype(jnp.bfloat16)
    qkv_out = (jnp.dot(normed, w_qkv, preferred_element_type=jnp.float32) + b_qkv.astype(jnp.float32)).astype(jnp.bfloat16)
    inv_freq = ROPE_BASE ** (-jnp.arange(0, ROT_DIMS, 2).astype(jnp.float32) / ROT_DIMS)
    angles = doc_pos.astype(jnp.float32)[:, None] * inv_freq[None, :]
    cos_q = jnp.cos(angles)[:, None, None, :]
    sin_q = jnp.sin(angles)[:, None, None, :]
    cos_k = jnp.cos(angles)[:, None, :]
    sin_k = jnp.sin(angles)[:, None, :]
    q_rot = rotate(qkv_out[:, :ATT_WIDTH].astype(jnp.float32).reshape(SEQ, GROUPS, REP_HEADS, HEAD), cos_q, sin_q).astype(jnp.bfloat16)
    k_rot = rotate(qkv_out[:, ATT_WIDTH:ATT_WIDTH + KV_WIDTH].astype(jnp.float32).reshape(SEQ, GROUPS, HEAD), cos_k, sin_k).astype(jnp.bfloat16)
    v_val = qkv_out[:, ATT_WIDTH + KV_WIDTH:].reshape(SEQ, GROUPS, HEAD)
    ctx_f32, attn_vjp = jax.vjp(
        lambda q_in, k_in, v_in: attention_core(q_in, k_in, v_in, seg_id),
        q_rot.astype(jnp.float32), k_rot.astype(jnp.float32), v_val.astype(jnp.float32))
    context = ctx_f32.astype(jnp.bfloat16).reshape(SEQ, ATT_WIDTH)
    y_out = (hid_f32 + jnp.dot(context, w_out, preferred_element_type=jnp.float32)).astype(jnp.bfloat16)
    grad_ctx = jnp.dot(grad_out, w_out.T, preferred_element_type=jnp.float32).astype(jnp.bfloat16)
    grad_wout = jnp.dot(context.T, grad_out, preferred_element_type=jnp.float32)
    d_query, d_key, d_value = attn_vjp(grad_ctx.astype(jnp.float32).reshape(SEQ, GROUPS, REP_HEADS, HEAD))
    grad_qkv = jnp.concatenate([
        rotate(d_query, cos_q, -sin_q).reshape(SEQ, ATT_WIDTH),
        rotate(d_key, cos_k, -sin_k).reshape(SEQ, KV_WIDTH),
        d_value.reshape(SEQ, KV_WIDTH)], axis=1).astype(jnp.bfloat16)
    grad_bqkv = jnp.sum(grad_qkv.astype(jnp.float32), axis=0)
    grad_wqkv = jnp.dot(normed.T, grad_qkv, preferred_element_type=jnp.float32)
    grad_normed = jnp.dot(grad_qkv, w_qkv.T, preferred_element_type=jnp.float32)
    grad_gain = jnp.sum(grad_normed * x_hat, axis=0)
    scaled = grad_normed * gain_f32
    grad_hidden = (grad_out.astype(jnp.float32) + inv_rms * (scaled - x_hat * jnp.mean(scaled * x_hat, axis=-1, keepdims=True))).astype(jnp.bfloat16)
    return (y_out, grad_hidden, grad_gain, grad_wqkv, grad_bqkv, grad_wout)
```

```python
import functools
import math

import jax
import jax.numpy as jnp
import numpy as np
from jax import lax
from jax.experimental import pallas as pl
from jax.experimental.pallas import tpu as pltpu
from jax.sharding import Mesh
from jax.sharding import PartitionSpec as P

HD = 128
ROT_DIMS = 64
ROPE_BASE = 5000000.0
EPS_NORM = 1e-5
NEG = -1e30
CORES = 2
SCALE = HD ** -0.5
CL2 = math.log2(math.e) * SCALE
f32, bf16 = jnp.float32, jnp.bfloat16
BQ, BK, LOOK_F, LOOK_B = 256, 256, 7, 4
VR = HD + 16
RISE = 60.0


def store_off(kb, bk, swap, piece):
    g = kb * bk
    pc = g // piece
    return (pc // 2) * (2 * piece) + ((pc % 2) ^ swap) * piece + g % piece


def visit_blocks(lo, hi, flo, fhi, block):
    @pl.loop(flo, fhi)
    def _(kb):
        block(kb, False)

    @pl.loop(0, (hi - lo) - (fhi - flo))
    def _(j):
        kb = lo + j
        block(jnp.where(kb < flo, kb, kb + (fhi - flo)), True)


def fwd_kernel(meta, q_ref, do_ref, kv_ref, qi_ref, ds_ref, ctx_ref, lse_ref, dd_ref, vt_ref, qt, m_s, mx, acc, vmax, *, nh, piece):
    i = pl.program_id(0)
    swap = meta[4, 0]
    lo, hi, flo, fhi = meta[0, i], meta[1, i], meta[2, i], meta[3, i]
    nk = kv_ref.shape[0]

    @pl.when(i == 0)
    def _():
        tail = jnp.where(lax.broadcasted_iota(jnp.int32, (VR - HD, 512), 0) == 0, 1.0, 0.0).astype(bf16)

        def step(c, m):
            at = pl.ds(pl.multiple_of(c * 512, 512), 512)
            v = kv_ref[at, HD:]
            vt_ref[:HD, at] = v.T
            vt_ref[HD:, at] = tail
            return jnp.maximum(m, jnp.max(jnp.abs(v.astype(f32)).reshape(64, 8, HD), axis=0))
        m = lax.fori_loop(0, nk // 512, step, jnp.zeros((8, HD), f32))
        vmax[...] = jnp.broadcast_to(jnp.max(m, keepdims=True), vmax.shape)

    for h in range(nh):
        qt[h] = q_ref[:, h * HD:(h + 1) * HD].T

    def load(kb):
        off = pl.multiple_of(store_off(kb, BK, swap, piece), BK)
        return kv_ref[pl.ds(off, BK), :HD], vt_ref[:, pl.ds(off, BK)]

    def visible(kb):
        kidx = kb * BK + lax.broadcasted_iota(jnp.int32, (BK, BQ), 0)
        return (kidx >= ds_ref[...]) & (kidx <= qi_ref[...])

    def heads(score, soft, pv):
        sc, pb = {}, {}
        for t in range(nh + LOOK_F + 1):
            if t < nh:
                sc[t] = score(t)
            if t >= LOOK_F + 1:
                pv(t - LOOK_F - 1, pb.pop(t - LOOK_F - 1))
            if LOOK_F <= t < nh + LOOK_F:
                pb[t - LOOK_F] = soft(t - LOOK_F, sc.pop(t - LOOK_F))

    def first(kb):
        kblk, vt = load(kb)
        msk = visible(kb)

        def score(h):
            return jnp.where(msk, jnp.dot(kblk, qt[h], preferred_element_type=f32) * CL2, 2 * NEG)

        def soft(h, s):
            m = jnp.max(s, axis=0, keepdims=True)
            m_s[h:h + 1, :] = m
            mx[h] = jnp.broadcast_to(m, (8, BQ))
            return jnp.exp2(s - m).astype(bf16)

        def pv(h, p):
            acc[h] = jnp.dot(vt, p, preferred_element_type=f32)

        heads(score, soft, pv)

    def block(kb, masked):
        kblk, vt = load(kb)
        msk = visible(kb) if masked else None

        def score(h):
            return jnp.dot(kblk, qt[h], preferred_element_type=f32) * CL2

        def soft(h, s):
            if masked:
                s = jnp.where(msk, s, 2 * NEG)
            mx[h] = jnp.maximum(mx[h], jnp.max(s.reshape(BK // 8, 8, BQ), axis=0))
            return jnp.exp2(s - m_s[h:h + 1, :]).astype(bf16)

        def pv(h, p):
            acc[h] += jnp.dot(vt, p, preferred_element_type=f32)

        heads(score, soft, pv)

    first(hi - 1)
    visit_blocks(lo, hi - 1, jnp.minimum(flo, jnp.minimum(fhi, hi - 1)), jnp.minimum(fhi, hi - 1), block)

    bad = jnp.zeros((8, BQ), f32)
    for h in range(nh):
        bad = jnp.maximum(bad, jnp.where(mx[h] - m_s[h:h + 1, :] <= RISE, 0.0, 1.0))
        bad = jnp.maximum(bad, jnp.where(acc[h, HD:HD + 1, :] * vmax[:1, :] <= 1e37, 0.0, 1.0))

    @pl.when(jnp.max(bad) > 0)
    def _():
        for h in range(nh):
            m_s[h:h + 1, :] = jnp.full((1, BQ), NEG, f32)
            acc[h] = jnp.zeros((VR, BQ), f32)

        @pl.loop(lo, hi)
        def _(kb):
            kblk, vt = load(kb)
            msk = visible(kb)
            for h in range(nh):
                s = jnp.where(msk, jnp.dot(kblk, qt[h], preferred_element_type=f32) * CL2, 2 * NEG)
                m_old = m_s[h:h + 1, :]
                m_new = jnp.maximum(m_old, jnp.max(s, axis=0, keepdims=True))
                m_s[h:h + 1, :] = m_new
                acc[h] = (acc[h] * jnp.exp2(m_old - m_new)
                          + jnp.dot(vt, jnp.exp2(s - m_new).astype(bf16), preferred_element_type=f32))

    for h in range(nh):
        lh = acc[h, HD:HD + 1, :]
        lse_ref[h:h + 1, :] = m_s[h:h + 1, :] + jnp.log2(lh)
        c = acc[h, :HD, :] * (1.0 / lh)
        dot_ = do_ref[:, h * HD:(h + 1) * HD].T.astype(f32)
        dd_ref[h:h + 1, :] = jnp.sum(c * dot_, axis=0, keepdims=True)
        ctx_ref[:, h * HD:(h + 1) * HD] = c.T.astype(bf16)


def resident(shape):
    return pl.BlockSpec(shape, lambda i, m: (0, 0), pipeline_mode=pl.Buffered(1))


def rows_spec(n):
    return pl.BlockSpec((n, BQ), lambda i, m: (0, i))


def flash_fwd(meta, q, do, kv, qi, ds, piece):
    t, w = q.shape
    nh = w // HD
    nk = kv.shape[0]
    tok = pl.BlockSpec((BQ, w), lambda i, m: (i, 0))
    gs = pltpu.PrefetchScalarGridSpec(
        num_scalar_prefetch=1, grid=(t // BQ,),
        in_specs=[tok, tok, resident((nk, 2 * HD)), rows_spec(1), rows_spec(1)],
        out_specs=[tok, rows_spec(nh), rows_spec(nh)],
        scratch_shapes=[pltpu.VMEM((VR, nk), bf16), pltpu.VMEM((nh, HD, BQ), bf16), pltpu.VMEM((nh, BQ), f32), pltpu.VMEM((nh, 8, BQ), f32),
                        pltpu.VMEM((nh, VR, BQ), f32), pltpu.VMEM((8, BQ), f32)])
    return pl.pallas_call(
        functools.partial(fwd_kernel, nh=nh, piece=piece), grid_spec=gs, name='flash_fwd',
        cost_estimate=pl.CostEstimate(flops=4 * t * t * w, bytes_accessed=t * w * 6, transcendentals=0),
        out_shape=[jax.ShapeDtypeStruct((t, w), bf16), jax.ShapeDtypeStruct((nh, t), f32),
                   jax.ShapeDtypeStruct((nh, t), f32)])(meta, q, do, kv, qi, ds)


def bwd_kernel(meta, q_ref, do_ref, kv_ref, qi_ref, ds_ref, lse_ref, dd_ref, tab_ref,
               dq_ref, dkv_ref, kt_ref, qt, dot_, dqa, *, nh, piece):
    i = pl.program_id(0)
    swap = meta[4, 0]

    @pl.when(i == 0)
    def _():
        def step(c, _):
            at = pl.ds(pl.multiple_of(c * 512, 512), 512)
            kt_ref[:, at] = kv_ref[at, :HD].T
            dkv_ref[at, :] = jnp.zeros((512, 2 * HD), f32)
            return 0
        lax.fori_loop(0, kv_ref.shape[0] // 512, step, 0)

    for h in range(nh):
        qt[h] = q_ref[:, h * HD:(h + 1) * HD].T
        dot_[h] = do_ref[:, h * HD:(h + 1) * HD].T
    dqa[...] = jnp.zeros_like(dqa)

    def block(kb, masked):
        off = pl.multiple_of(store_off(kb, BK, swap, piece), BK)
        kblk = kv_ref[pl.ds(off, BK), :HD]
        kt = kt_ref[:, pl.ds(off, BK)]
        vblk = kv_ref[pl.ds(off, BK), HD:]
        if masked:
            kidx = kb * BK + lax.broadcasted_iota(jnp.int32, (BK, BQ), 0)
            msk = (kidx >= ds_ref[...]) & (kidx <= qi_ref[...])
        acc = [None, None]

        def mid(h, s, dp):
            p = jnp.exp2(s * CL2 - lse_ref[h:h + 1, :])
            if masked:
                p = jnp.where(msk, p, 0.0)
            return p.astype(bf16), (p * (dp - dd_ref[h:h + 1, :])).astype(bf16)

        sc, pa = {}, {}
        for t in range(nh + LOOK_B + 1):
            if t < nh:
                sc[t] = (jnp.dot(kblk, qt[t], preferred_element_type=f32),
                         jnp.dot(vblk, dot_[t], preferred_element_type=f32))
            u = t - LOOK_B - 1
            if u >= 0:
                pb, dsb = pa.pop(u)
                t1 = jnp.dot(pb, do_ref[:, u * HD:(u + 1) * HD], preferred_element_type=f32)
                t2 = jnp.dot(dsb, q_ref[:, u * HD:(u + 1) * HD], preferred_element_type=f32)
                acc[0] = t1 if acc[0] is None else acc[0] + t1
                acc[1] = t2 if acc[1] is None else acc[1] + t2
                dqa[u] += jnp.dot(kt, dsb, preferred_element_type=f32)
            if LOOK_B <= t < nh + LOOK_B:
                pa[t - LOOK_B] = mid(t - LOOK_B, *sc.pop(t - LOOK_B))
        dkv_ref[pl.ds(off, BK), :HD] += acc[1]
        dkv_ref[pl.ds(off, BK), HD:] += acc[0]

    visit_blocks(meta[0, i], meta[1, i], meta[2, i], meta[3, i], block)
    ct = tab_ref[:, :HD].T
    even = lax.broadcasted_iota(jnp.int32, (HD, BQ), 0) % 2 == 0
    st = jnp.where(even, tab_ref[:, HD:].T, -tab_ref[:, HD:].T)
    for h in range(nh):
        g = dqa[h] * SCALE
        part = jnp.where(even, pltpu.roll(g, HD - 1, 0), pltpu.roll(g, 1, 0))
        dq_ref[:, h * HD:(h + 1) * HD] = (g * ct + part * st).T.astype(bf16)


def flash_bwd(meta, q, do, kv, qi, ds, lse, dd, tab, piece):
    t, w = q.shape
    nh = w // HD
    nk = kv.shape[0]
    tok = pl.BlockSpec((BQ, w), lambda i, m: (i, 0))
    gs = pltpu.PrefetchScalarGridSpec(
        num_scalar_prefetch=1, grid=(t // BQ,),
        in_specs=[tok, tok, resident((nk, 2 * HD)), rows_spec(1), rows_spec(1),
                  rows_spec(nh), rows_spec(nh), pl.BlockSpec((BQ, 2 * HD), lambda i, m: (i, 0))],
        out_specs=[tok, resident((nk, 2 * HD))],
        scratch_shapes=[pltpu.VMEM((HD, nk), bf16), pltpu.VMEM((nh, HD, BQ), bf16), pltpu.VMEM((nh, HD, BQ), bf16), pltpu.VMEM((nh, HD, BQ), f32)])
    return pl.pallas_call(
        functools.partial(bwd_kernel, nh=nh, piece=piece), grid_spec=gs, name='flash_bwd',
        cost_estimate=pl.CostEstimate(flops=10 * t * t * w, bytes_accessed=t * w * 8, transcendentals=0),
        out_shape=[jax.ShapeDtypeStruct((t, w), bf16), jax.ShapeDtypeStruct((nk, 2 * HD), f32)],
    )(meta, q, do, kv, qi, ds, lse, dd, tab)


MESH = pl.DeviceIdType.MESH


def front_kernel(hid, go, tab, gain_ref, b_ref, rot_ref, w_qkv, w_out,
                 normed, go_o, q_out, gctx_out, kv_all, tab2,
                 hid_v, go_v, tab_v, nrm_v, w_v, wo_v, q_v, gc_v, kv_v,
                 loc, ssem, rsem, ksend, krecv, *, n, nx, aw, kw, att):
    x, k = lax.axis_index('x'), lax.axis_index('k')
    right, left = lax.rem(x + 1, nx), lax.rem(x + nx - 1, nx)
    bar = pltpu.get_barrier_semaphore()
    for peer in ({'k': 1 - k}, {'x': right}, {'x': left}):
        pl.semaphore_signal(bar, inc=1, device_id=peer, device_id_type=MESH)

    kvw = CORES * kw
    col = lambda at, size: w_qkv.at[:, pl.ds(pl.multiple_of(at, HD), size)]
    loads = [pltpu.make_async_copy(hid, hid_v.at[0], loc.at[0]),
             pltpu.make_async_copy(col(att + k * kw, kw), w_v.at[:, aw:aw + kw], loc.at[1]),
             pltpu.make_async_copy(col(att + kvw + k * kw, kw), w_v.at[:, aw + kw:], loc.at[2]),
             pltpu.make_async_copy(tab, tab_v.at[0], loc.at[3]),
             pltpu.make_async_copy(col(k * aw, aw), w_v.at[:, :aw], loc.at[4]),
             pltpu.make_async_copy(go, go_v.at[0], loc.at[5]),
             pltpu.make_async_copy(w_out.at[pl.ds(pl.multiple_of(k * aw, aw), aw), :], wo_v, loc.at[6])]
    for c in loads:
        c.start()
    pl.semaphore_wait(bar, 3)
    give = [pltpu.make_async_remote_copy(src, dst.at[1], ssem.at[i], rsem.at[i], device_id={'k': 1 - k}, device_id_type=MESH)
            for i, (src, dst) in enumerate(((hid, hid_v), (tab, tab_v), (go, go_v)))]
    for c in give:
        c.start()

    gain = gain_ref[...].astype(f32)
    bias = jnp.where(k == 0, b_ref[0:1, :], b_ref[1:2, :])
    rot = rot_ref[...]
    tile = 256
    ntile = n // tile
    full_rows = lambda c, p: pl.ds(pl.multiple_of(c * (2 * n) + p * n, n), n)

    def rope(v, p, r):
        ct = tab_v[p, pl.ds(r, tile), :HD]
        st = tab_v[p, pl.ds(r, tile), HD:]
        return (v.astype(f32) * ct + jnp.dot(v, rot, preferred_element_type=f32) * st).astype(bf16)

    def keys(p):
        def body(t, _):
            r = pl.multiple_of(t * tile, tile)
            h = hid_v[p, pl.ds(r, tile), :].astype(f32)
            inv = lax.rsqrt(jnp.mean(h * h, axis=-1, keepdims=True) + EPS_NORM)
            nv = (h * inv * gain).astype(bf16)
            nrm_v[pl.ds(p * n + r, tile), :] = nv
            kv = (jnp.dot(nv, w_v[:, aw:], preferred_element_type=f32) + bias[:, aw:]).astype(bf16)
            kv_v[pl.ds(p * n + r, tile), :kw] = rope(kv[:, :kw], p, r)
            kv_v[pl.ds(p * n + r, tile), kw:] = kv[:, kw:]
            return 0
        lax.fori_loop(0, ntile, body, 0)

    def queries(p):
        def body(t, _):
            r = pl.multiple_of(t * tile, tile)
            qv = (jnp.dot(nrm_v[pl.ds(p * n + r, tile), :], w_v[:, :aw], preferred_element_type=f32) + bias[:, :aw]).astype(bf16)
            for h in range(aw // HD):
                q_v[pl.ds(p * n + r, tile), h * HD:(h + 1) * HD] = rope(qv[:, h * HD:(h + 1) * HD], p, r)
            return 0
        lax.fori_loop(0, ntile, body, 0)

    def grads(p):
        def body(t, _):
            r = pl.multiple_of(t * tile, tile)
            gc_v[pl.ds(p * n + r, tile), :] = lax.dot_general(
                go_v[p, pl.ds(r, tile), :], wo_v[...], (((1,), (1,)), ((), ())), preferred_element_type=f32).astype(bf16)
            return 0
        lax.fori_loop(0, ntile, body, 0)

    def spread_kv(p):
        out = []
        for d, peer in enumerate((right, left)):
            c = pltpu.make_async_remote_copy(kv_v.at[p * n:(p + 1) * n, :], kv_all.at[full_rows(x, p), :],
                                             ksend.at[2 * p + d], krecv.at[2 * p + d], device_id={'x': peer}, device_id_type=MESH)
            c.start()
            out.append(c)
        return out

    for c in loads[:4]:
        c.wait()
    keys(0)
    sent = spread_kv(0)
    give[0].wait_recv()
    give[1].wait_recv()
    keys(1)
    sent += spread_kv(1)
    stores = [pltpu.make_async_copy(kv_v, kv_all.at[pl.ds(pl.multiple_of(x * (2 * n), 2 * n), 2 * n), :], loc.at[7]),
              pltpu.make_async_copy(nrm_v, normed, loc.at[8]),
              pltpu.make_async_copy(tab_v.at[0], tab2.at[0:n, :], loc.at[9]),
              pltpu.make_async_copy(tab_v.at[1], tab2.at[n:, :], loc.at[10])]
    for c in stores:
        c.start()
    loads[4].wait()
    queries(0)

    sent[0].wait_recv()
    on0 = pltpu.make_async_remote_copy(kv_all.at[full_rows(left, 0), :], kv_all.at[full_rows(left, 0), :],
                                       ksend.at[4], krecv.at[4], device_id={'x': right}, device_id_type=MESH)
    on0.start()
    queries(1)
    stores.append(pltpu.make_async_copy(q_v, q_out, loc.at[11]))
    stores[-1].start()
    sent[3].wait_recv()
    on1 = pltpu.make_async_remote_copy(kv_all.at[full_rows(right, 1), :], kv_all.at[full_rows(right, 1), :],
                                       ksend.at[5], krecv.at[5], device_id={'x': left}, device_id_type=MESH)
    on1.start()
    loads[5].wait()
    loads[6].wait()
    grads(0)
    give[2].wait_recv()
    stores.append(pltpu.make_async_copy(go_v.at[1], go_o, loc.at[12]))
    stores[-1].start()
    grads(1)
    stores.append(pltpu.make_async_copy(gc_v, gctx_out, loc.at[13]))
    stores[-1].start()
    for c in stores:
        c.wait()
    for c in give:
        c.wait_send()
    sent[1].wait_recv()
    sent[2].wait_recv()
    for c in sent:
        c.wait_send()
    on0.wait()
    on1.wait()


def front(hidden, grad_out, tab, norm_gain, bias, rot, w_qkv, w_out, nx, kw):
    n, d = hidden.shape
    att = w_out.shape[0]
    aw = att // CORES
    hbm = pl.BlockSpec(memory_space=pl.ANY)
    vmem = pl.BlockSpec(memory_space=pltpu.VMEM)
    sds = jax.ShapeDtypeStruct
    dma = pltpu.SemaphoreType.DMA
    return pl.pallas_call(
        functools.partial(front_kernel, n=n, nx=nx, aw=aw, kw=kw, att=att), name='front',
        in_specs=[hbm, hbm, hbm, vmem, vmem, vmem, hbm, hbm], out_specs=[hbm] * 6,
        out_shape=[sds((2 * n, d), bf16), sds((n, d), bf16), sds((2 * n, aw), bf16), sds((2 * n, aw), bf16),
                   sds((nx * 2 * n, 2 * kw), bf16), sds((2 * n, 2 * HD), f32)],
        scratch_shapes=[pltpu.VMEM((2, n, d), bf16), pltpu.VMEM((2, n, d), bf16), pltpu.VMEM((2, n, 2 * HD), f32),
                        pltpu.VMEM((2 * n, d), bf16), pltpu.VMEM((d, aw + 2 * kw), bf16), pltpu.VMEM((aw, d), bf16),
                        pltpu.VMEM((2 * n, aw), bf16), pltpu.VMEM((2 * n, aw), bf16), pltpu.VMEM((2 * n, 2 * kw), bf16),
                        dma((14,)), dma((3,)), dma((3,)), dma((6,)), dma((6,))],
        compiler_params=pltpu.CompilerParams(collective_id=0, has_side_effects=True, vmem_limit_bytes=60 << 20),
        cost_estimate=pl.CostEstimate(flops=60 * 10 ** 9, bytes_accessed=50 * 10 ** 6, transcendentals=0),
    )(hidden, grad_out, tab, norm_gain, bias, rot, w_qkv, w_out)


def block_table(qi, ds, swap):
    q2, d2 = qi.reshape(-1, BQ), ds.reshape(-1, BQ)
    lo = d2[:, 0] // BK
    hi = q2[:, -1] // BK + 1
    flo = jnp.minimum((d2[:, -1] + BK - 1) // BK, hi)
    fhi = jnp.maximum((q2[:, 0] + 1) // BK, flo)
    return jnp.stack([lo, hi, flo, fhi, jnp.full_like(lo, swap)]).astype(jnp.int32)


def pair_swap():
    r = np.zeros((HD, HD), np.float32)
    for j in range(ROT_DIMS // 2):
        r[2 * j + 1, 2 * j] = -1.0
        r[2 * j, 2 * j + 1] = 1.0
    return r


def solution(mesh):
    axes = dict(mesh.shape)
    mesh3 = Mesh(mesh.devices.reshape(axes['dp'], axes['cp'] // CORES, CORES), ('dp', 'x', 'k'))
    flip = [(0, 1), (1, 0)]
    nx = mesh3.shape['x']

    def per_device(hidden, seg_id, doc_pos, norm_gain, w_qkv, b_qkv, w_out, grad_out):
        n, d = hidden.shape
        att = w_out.shape[0]
        kvw = (w_qkv.shape[1] - att) // 2
        aw, kw = att // CORES, kvw // CORES
        x, k = lax.axis_index('x'), lax.axis_index('k')
        other = lambda a: lax.ppermute(a, 'k', flip)
        both = lambda a: jnp.concatenate([a, other(a)], axis=0)

        pos2 = both(doc_pos)
        base = x * (CORES * n)
        qi = jnp.concatenate([base + k * n + jnp.arange(n), base + (1 - k) * n + jnp.arange(n)]).astype(jnp.int32)
        ds = qi - pos2
        meta = block_table(qi, ds, k)

        def cols(w, c):
            part = lambda a, b: lax.dynamic_slice_in_dim(w, a, b, axis=-1)
            return jnp.concatenate([part(c * aw, aw), part(att + c * kw, kw), part(att + kvw + c * kw, kw)], axis=-1)

        inv_freq = ROPE_BASE ** (-jnp.arange(0, ROT_DIMS, 2).astype(f32) / ROT_DIMS)
        ang = inv_freq[:, None] * doc_pos.astype(f32)[None, :]
        wide = lambda a, fill: jnp.concatenate([jnp.repeat(a, 2, axis=0), jnp.full((HD - ROT_DIMS, n), fill, f32)], axis=0)
        tab = jnp.concatenate([wide(jnp.cos(ang), 1.0), wide(jnp.sin(ang), 0.0)], axis=0).T
        bias = jnp.stack([jnp.concatenate([b_qkv[c * aw:(c + 1) * aw], b_qkv[att + c * kw:att + (c + 1) * kw],
                                           b_qkv[att + kvw + c * kw:att + kvw + (c + 1) * kw]]) for c in range(CORES)]).astype(f32)
        gain = norm_gain.astype(f32)
        normed, go_o, q, gctx, kv_all, tab2 = front(hidden, grad_out, tab, norm_gain[None], bias,
                                                     jnp.asarray(pair_swap(), bf16), w_qkv, w_out, nx, kw)
        w_me, w_ot = cols(w_qkv, k), cols(w_qkv, 1 - k)
        wo_me = lax.dynamic_slice_in_dim(w_out, k * aw, aw, axis=0)
        wo_ot = lax.dynamic_slice_in_dim(w_out, (1 - k) * aw, aw, axis=0)
        ctx, lse, dd = flash_fwd(meta, q, gctx, kv_all, qi[None], ds[None], n)
        over = (((0,), (0,)), ((), ()))
        g_wout = (lax.dot_general(ctx[:n], grad_out, over, preferred_element_type=f32)
                  + lax.dot_general(ctx[n:], go_o, over, preferred_element_type=f32))
        lse, g_wout = lax.optimization_barrier((lse, g_wout))
        g_wout = lax.psum(g_wout, 'x')
        ctx_o = other(ctx[n:])
        y_out = (hidden.astype(f32) + jnp.dot(ctx[:n], wo_me, preferred_element_type=f32)
                 + jnp.dot(ctx_o, wo_ot, preferred_element_type=f32)).astype(bf16)

        dq, dkv = flash_bwd(meta, q, gctx, kv_all, qi[None], ds[None], lse, dd, tab2, n)
        c_tok, s_tok = tab2[:, :HD], tab2[:, HD:]
        dkv, g_wout = lax.optimization_barrier((dkv, g_wout))
        wout_o = other(g_wout)
        o_wout = jnp.where(k == 0, jnp.concatenate([g_wout, wout_o]), jnp.concatenate([wout_o, g_wout]))
        dkv = lax.psum_scatter(dkv, 'x', scatter_dimension=0, tiled=True)
        dk = dkv[:, :kw] * SCALE
        dkt = jnp.dot(dk, jnp.asarray(pair_swap().T), precision=lax.Precision.HIGHEST, preferred_element_type=f32)
        gqkv = jnp.concatenate([dq, (dk * c_tok + dkt * s_tok).astype(bf16), dkv[:, kw:].astype(bf16)], axis=1)
        g_wqkv = lax.dot_general(normed, gqkv, (((0,), (0,)), ((), ())), preferred_element_type=f32)
        g_wqkv = lax.psum_scatter(g_wqkv, 'x', scatter_dimension=0, tiled=True)
        g_wqkv = lax.all_gather(g_wqkv, ('x', 'k'), axis=0)
        g_wqkv = g_wqkv.reshape(-1, CORES, *g_wqkv.shape[1:])
        two = lambda a, b: [g_wqkv[:, c, :, a:b] for c in range(CORES)]
        o_wqkv = jnp.concatenate(two(0, aw) + two(aw, aw + kw) + two(aw + kw, aw + 2 * kw), axis=-1).reshape(w_qkv.shape)
        gq_o = other(gqkv[n:])
        dims = (((1,), (1,)), ((), ()))
        gnorm = (lax.dot_general(gqkv[:n], w_me, dims, preferred_element_type=f32)
                 + lax.dot_general(gq_o, w_ot, dims, preferred_element_type=f32))
        h32 = hidden.astype(f32)
        inv_rms = lax.rsqrt(jnp.mean(h32 * h32, axis=-1, keepdims=True) + EPS_NORM)
        x_hat = h32 * inv_rms
        g_gain = jnp.sum(gnorm * x_hat, axis=0)
        scaled = gnorm * gain
        g_hidden = (grad_out.astype(f32) + inv_rms * (scaled - x_hat * jnp.mean(scaled * x_hat, axis=-1, keepdims=True))).astype(bf16)
        g_b = jnp.sum(gqkv.astype(f32), axis=0)
        g_gain = lax.psum(g_gain, ('x', 'k'))
        g_b = lax.psum(g_b, 'x')

        def join(out, mine, c):
            put = lambda o, v, at: lax.dynamic_update_slice_in_dim(o, v, at, axis=-1)
            out = put(out, mine[..., :aw], c * aw)
            out = put(out, mine[..., aw:aw + kw], att + c * kw)
            return put(out, mine[..., aw + kw:], att + kvw + c * kw)

        full = lambda shape: jnp.zeros(shape, f32)
        o_b = join(join(full(b_qkv.shape), g_b, k), other(g_b), 1 - k)
        return y_out, g_hidden, g_gain, o_wqkv, o_b, o_wout

    act = P(('dp', 'x', 'k'), None)
    row = P(('dp', 'x', 'k'))
    return jax.shard_map(per_device, mesh=mesh3,
                         in_specs=(act, row, row, P(), P(), P(), P(), act),
                         out_specs=(act, act, P('dp'), P('dp', None), P('dp'), P('dp', None)),
                         check_vma=False)
```

```python
import functools
import math

import jax
import jax.numpy as jnp
import numpy as np
from jax import lax
from jax.experimental import pallas as pl
from jax.experimental.pallas import tpu as pltpu
from jax.sharding import Mesh
from jax.sharding import PartitionSpec as P

HD = 128
ROT_DIMS = 64
ROPE_BASE = 5000000.0
EPS_NORM = 1e-5
NEG = -1e30
CORES = 2
SCALE = HD ** -0.5
CL2 = math.log2(math.e) * SCALE
f32, bf16 = jnp.float32, jnp.bfloat16
BQ, BK, LOOK_F, LOOK_B = 256, 256, 3, 4
VR = HD + 16
RISE = 60.0


def store_off(kb, bk, swap, piece):
    g = kb * bk
    pc = g // piece
    return (pc // 2) * (2 * piece) + ((pc % 2) ^ swap) * piece + g % piece


def visit_blocks(lo, hi, flo, fhi, block):
    pairs = (fhi - flo) // 2

    @pl.loop(0, pairs)
    def _(j):
        block((flo + 2 * j, flo + 2 * j + 1), False)

    @pl.when(flo + 2 * pairs < fhi)
    def _():
        block((fhi - 1,), False)

    @pl.loop(0, (hi - lo) - (fhi - flo))
    def _(j):
        kb = lo + j
        block((jnp.where(kb < flo, kb, kb + (fhi - flo)),), True)


def fwd_kernel(meta, q_ref, do_ref, kv_ref, qi_ref, ds_ref, ctx_ref, lse_ref, dd_ref, vt_ref, qt, m_s, mx, acc, vmax, *, nh, piece):
    i = pl.program_id(0)
    swap = meta[4, 0]
    lo, hi, flo, fhi = meta[0, i], meta[1, i], meta[2, i], meta[3, i]
    nk = kv_ref.shape[0]

    @pl.when(i == 0)
    def _():
        tail = jnp.where(lax.broadcasted_iota(jnp.int32, (VR - HD, 512), 0) == 0, 1.0, 0.0).astype(bf16)

        def step(c, m):
            at = pl.ds(pl.multiple_of(c * 512, 512), 512)
            v = kv_ref[at, HD:]
            vt_ref[:HD, at] = v.T
            vt_ref[HD:, at] = tail
            return jnp.maximum(m, jnp.max(jnp.abs(v.astype(f32)).reshape(64, 8, HD), axis=0))
        m = lax.fori_loop(0, nk // 512, step, jnp.zeros((8, HD), f32))
        vmax[...] = jnp.broadcast_to(jnp.max(m, keepdims=True), vmax.shape)

    for h in range(nh):
        qt[h] = q_ref[:, h * HD:(h + 1) * HD].T

    def load(kb):
        off = pl.multiple_of(store_off(kb, BK, swap, piece), BK)
        return kv_ref[pl.ds(off, BK), :HD], vt_ref[:, pl.ds(off, BK)]

    def visible(kb):
        kidx = kb * BK + lax.broadcasted_iota(jnp.int32, (BK, BQ), 0)
        return (kidx >= ds_ref[...]) & (kidx <= qi_ref[...])

    def units(n_units, score, soft, pv):
        la = LOOK_F if n_units > nh else nh - 1
        sc, pb = {}, {}
        for t in range(n_units + la + 1):
            if t < n_units:
                sc[t] = score(t)
            if t >= la + 1:
                pv(t - la - 1, pb.pop(t - la - 1))
            if la <= t < n_units + la:
                pb[t - la] = soft(t - la, sc.pop(t - la))

    def first(kb):
        kblk, vt = load(kb)
        msk = visible(kb)

        def score(h):
            return jnp.where(msk, jnp.dot(kblk, qt[h], preferred_element_type=f32) * CL2, 2 * NEG)

        def soft(h, s):
            m = jnp.max(s, axis=0, keepdims=True)
            m_s[h:h + 1, :] = m
            mx[h] = jnp.broadcast_to(m, (8, BQ))
            return jnp.exp2(s - m).astype(bf16)

        def pv(h, p):
            acc[h] = jnp.dot(vt, p, preferred_element_type=f32)

        units(nh, score, soft, pv)

    def block(kbs, masked):
        kv = [load(kb) for kb in kbs]
        msk = visible(kbs[0]) if masked else None

        def score(u):
            return jnp.dot(kv[u // nh][0], qt[u % nh], preferred_element_type=f32) * CL2

        def soft(u, s):
            h = u % nh
            if masked:
                s = jnp.where(msk, s, 2 * NEG)
            mx[h] = jnp.maximum(mx[h], jnp.max(s.reshape(BK // 8, 8, BQ), axis=0))
            return jnp.exp2(s - m_s[h:h + 1, :]).astype(bf16)

        def pv(u, p):
            acc[u % nh] += jnp.dot(kv[u // nh][1], p, preferred_element_type=f32)

        units(nh * len(kbs), score, soft, pv)

    first(hi - 1)
    visit_blocks(lo, hi - 1, jnp.minimum(flo, jnp.minimum(fhi, hi - 1)), jnp.minimum(fhi, hi - 1), block)

    bad = jnp.zeros((8, BQ), f32)
    for h in range(nh):
        bad = jnp.maximum(bad, jnp.where(mx[h] - m_s[h:h + 1, :] <= RISE, 0.0, 1.0))
        bad = jnp.maximum(bad, jnp.where(acc[h, HD:HD + 1, :] * vmax[:1, :] <= 1e37, 0.0, 1.0))

    @pl.when(jnp.max(bad) > 0)
    def _():
        for h in range(nh):
            m_s[h:h + 1, :] = jnp.full((1, BQ), NEG, f32)
            acc[h] = jnp.zeros((VR, BQ), f32)

        @pl.loop(lo, hi)
        def _(kb):
            kblk, vt = load(kb)
            msk = visible(kb)
            for h in range(nh):
                s = jnp.where(msk, jnp.dot(kblk, qt[h], preferred_element_type=f32) * CL2, 2 * NEG)
                m_old = m_s[h:h + 1, :]
                m_new = jnp.maximum(m_old, jnp.max(s, axis=0, keepdims=True))
                m_s[h:h + 1, :] = m_new
                acc[h] = (acc[h] * jnp.exp2(m_old - m_new)
                          + jnp.dot(vt, jnp.exp2(s - m_new).astype(bf16), preferred_element_type=f32))

    for h in range(nh):
        lh = acc[h, HD:HD + 1, :]
        lse_ref[h:h + 1, :] = m_s[h:h + 1, :] + jnp.log2(lh)
        c = acc[h, :HD, :] * (1.0 / lh)
        dot_ = do_ref[:, h * HD:(h + 1) * HD].T.astype(f32)
        dd_ref[h:h + 1, :] = jnp.sum(c * dot_, axis=0, keepdims=True)
        ctx_ref[:, h * HD:(h + 1) * HD] = c.T.astype(bf16)


def resident(shape):
    return pl.BlockSpec(shape, lambda i, m: (0, 0), pipeline_mode=pl.Buffered(1))


def rows_spec(n):
    return pl.BlockSpec((n, BQ), lambda i, m: (0, i))


def flash_fwd(meta, q, do, kv, qi, ds, piece):
    t, w = q.shape
    nh = w // HD
    nk = kv.shape[0]
    tok = pl.BlockSpec((BQ, w), lambda i, m: (i, 0))
    gs = pltpu.PrefetchScalarGridSpec(
        num_scalar_prefetch=1, grid=(t // BQ,),
        in_specs=[tok, tok, resident((nk, 2 * HD)), rows_spec(1), rows_spec(1)],
        out_specs=[tok, rows_spec(nh), rows_spec(nh)],
        scratch_shapes=[pltpu.VMEM((VR, nk), bf16), pltpu.VMEM((nh, HD, BQ), bf16), pltpu.VMEM((nh, BQ), f32), pltpu.VMEM((nh, 8, BQ), f32),
                        pltpu.VMEM((nh, VR, BQ), f32), pltpu.VMEM((8, BQ), f32)])
    return pl.pallas_call(
        functools.partial(fwd_kernel, nh=nh, piece=piece), grid_spec=gs, name='flash_fwd',
        cost_estimate=pl.CostEstimate(flops=4 * t * t * w, bytes_accessed=t * w * 6, transcendentals=0),
        out_shape=[jax.ShapeDtypeStruct((t, w), bf16), jax.ShapeDtypeStruct((nh, t), f32),
                   jax.ShapeDtypeStruct((nh, t), f32)])(meta, q, do, kv, qi, ds)


def bwd_kernel(meta, q_ref, do_ref, kv_ref, qi_ref, ds_ref, lse_ref, dd_ref, *rest, nh, piece, near):
    if near:
        tab_ref, dq_in, dq_ref, dkv_ref, kt_ref, qt, dot_, dqa = rest
    else:
        dqa, dkv_ref, kt_ref, qt, dot_ = rest
    i = pl.program_id(0)
    swap = meta[4, 0]

    @pl.when(i == 0)
    def _():
        def step(c, _):
            at = pl.ds(pl.multiple_of(c * 512, 512), 512)
            kt_ref[:, at] = kv_ref[at, :HD].T
            dkv_ref[at, :] = jnp.zeros((512, 2 * HD), f32)
            return 0
        lax.fori_loop(0, kv_ref.shape[0] // 512, step, 0)

    for h in range(nh):
        qt[h] = q_ref[:, h * HD:(h + 1) * HD].T
        dot_[h] = do_ref[:, h * HD:(h + 1) * HD].T
    dqa[...] = dq_in[...] if near else jnp.zeros_like(dqa)

    def block(kbs, masked):
        base = meta[5, 0] * (2 * piece) if near else 0
        at = [pl.ds(pl.multiple_of(store_off(kb, BK, swap, piece) - base, BK), BK) for kb in kbs]
        if masked:
            kidx = kbs[0] * BK + lax.broadcasted_iota(jnp.int32, (BK, BQ), 0)
            msk = (kidx >= ds_ref[...]) & (kidx <= qi_ref[...])
        acc = {}

        def mid(h, s, dp):
            p = jnp.exp2(s * CL2 - lse_ref[h:h + 1, :])
            if masked:
                p = jnp.where(msk, p, 0.0)
            return p.astype(bf16), (p * (dp - dd_ref[h:h + 1, :])).astype(bf16)

        def add(key, v):
            acc[key] = v if key not in acc else acc[key] + v

        sc, pa = {}, {}
        n_units = nh * len(kbs)
        for t in range(n_units + LOOK_B + 1):
            if t < n_units:
                b, h = divmod(t, nh)
                sc[t] = (jnp.dot(kv_ref[at[b], :HD], qt[h], preferred_element_type=f32),
                         jnp.dot(kv_ref[at[b], HD:], dot_[h], preferred_element_type=f32))
            u = t - LOOK_B - 1
            if u >= 0:
                b, h = divmod(u, nh)
                pb, dsb = pa.pop(u)
                add((b, 1), jnp.dot(pb, do_ref[:, h * HD:(h + 1) * HD], preferred_element_type=f32))
                add((b, 0), jnp.dot(dsb, q_ref[:, h * HD:(h + 1) * HD], preferred_element_type=f32))
                dqa[h] += jnp.dot(kt_ref[:, at[b]], dsb, preferred_element_type=f32)
            if LOOK_B <= t < n_units + LOOK_B:
                pa[t - LOOK_B] = mid((t - LOOK_B) % nh, *sc.pop(t - LOOK_B))
        for b in range(len(kbs)):
            dkv_ref[at[b], :HD] += acc[b, 0]
            dkv_ref[at[b], HD:] += acc[b, 1]

    split = meta[5, 0] * (2 * piece // BK)
    clip = (lambda v: jnp.maximum(v, split)) if near else (lambda v: jnp.minimum(v, split))
    visit_blocks(*[clip(meta[r, i]) for r in range(4)], block)
    if near:
        ct = tab_ref[:, :HD].T
        even = lax.broadcasted_iota(jnp.int32, (HD, BQ), 0) % 2 == 0
        st = jnp.where(even, tab_ref[:, HD:].T, -tab_ref[:, HD:].T)
        for h in range(nh):
            g = dqa[h] * SCALE
            part = jnp.where(even, pltpu.roll(g, HD - 1, 0), pltpu.roll(g, 1, 0))
            dq_ref[:, h * HD:(h + 1) * HD] = (g * ct + part * st).T.astype(bf16)


def flash_bwd(meta, q, do, kv, qi, ds, lse, dd, piece, tab=None, dq=None):
    near = tab is not None
    t, w = q.shape
    nh = w // HD
    nk = 2 * piece if near else kv.shape[0]
    tok = pl.BlockSpec((BQ, w), lambda i, m: (i, 0))
    dqs = pl.BlockSpec((None, nh, HD, BQ), lambda i, m: (i, 0, 0, 0))
    keys = pl.BlockSpec((nk, 2 * HD), lambda i, m: (m[5, 0] if near else 0, 0), pipeline_mode=pl.Buffered(1))
    part = jax.ShapeDtypeStruct((t // BQ, nh, HD, BQ), f32)
    gs = pltpu.PrefetchScalarGridSpec(
        num_scalar_prefetch=1, grid=(t // BQ,),
        in_specs=[tok, tok, keys, rows_spec(1), rows_spec(1), rows_spec(nh), rows_spec(nh)]
        + ([pl.BlockSpec((BQ, 2 * HD), lambda i, m: (i, 0)), dqs] if near else []),
        out_specs=[tok if near else dqs, resident((nk, 2 * HD))],
        scratch_shapes=[pltpu.VMEM((HD, nk), bf16), pltpu.VMEM((nh, HD, BQ), bf16), pltpu.VMEM((nh, HD, BQ), bf16)]
        + ([pltpu.VMEM((nh, HD, BQ), f32)] if near else []))
    return pl.pallas_call(
        functools.partial(bwd_kernel, nh=nh, piece=piece, near=near), grid_spec=gs, name='flash_bwd_' + ('near' if near else 'far'),
        cost_estimate=pl.CostEstimate(flops=(4 if near else 7) * t * t * w, bytes_accessed=t * w * 8, transcendentals=0),
        out_shape=[jax.ShapeDtypeStruct((t, w), bf16) if near else part, jax.ShapeDtypeStruct((nk, 2 * HD), f32)],
    )(meta, q, do, kv, qi, ds, lse, dd, *((tab, dq) if near else ()))


MESH = pl.DeviceIdType.MESH


def front_kernel(hid, go, tab, gain_ref, b_ref, rot_ref, w_qkv, w_out,
                 normed, go_o, q_out, gctx_out, kv_all, tab2,
                 hid_v, go_v, tab_v, nrm_v, w_v, wo_v, q_v, gc_v, kv_v,
                 loc, ssem, rsem, ksend, krecv, *, n, nx, aw, kw, att):
    x, k = lax.axis_index('x'), lax.axis_index('k')
    right, left = lax.rem(x + 1, nx), lax.rem(x + nx - 1, nx)
    bar = pltpu.get_barrier_semaphore()
    for peer in ({'k': 1 - k}, {'x': right}, {'x': left}):
        pl.semaphore_signal(bar, inc=1, device_id=peer, device_id_type=MESH)

    kvw = CORES * kw
    col = lambda at, size: w_qkv.at[:, pl.ds(pl.multiple_of(at, HD), size)]
    loads = [pltpu.make_async_copy(hid, hid_v.at[0], loc.at[0]),
             pltpu.make_async_copy(col(att + k * kw, kw), w_v.at[:, aw:aw + kw], loc.at[1]),
             pltpu.make_async_copy(col(att + kvw + k * kw, kw), w_v.at[:, aw + kw:], loc.at[2]),
             pltpu.make_async_copy(tab, tab_v.at[0], loc.at[3]),
             pltpu.make_async_copy(col(k * aw, aw), w_v.at[:, :aw], loc.at[4]),
             pltpu.make_async_copy(go, go_v.at[0], loc.at[5]),
             pltpu.make_async_copy(w_out.at[pl.ds(pl.multiple_of(k * aw, aw), aw), :], wo_v, loc.at[6])]
    for c in loads:
        c.start()
    pl.semaphore_wait(bar, 3)
    give = [pltpu.make_async_remote_copy(src, dst.at[1], ssem.at[i], rsem.at[i], device_id={'k': 1 - k}, device_id_type=MESH)
            for i, (src, dst) in enumerate(((hid, hid_v), (tab, tab_v), (go, go_v)))]
    for c in give:
        c.start()

    gain = gain_ref[...].astype(f32)
    bias = jnp.where(k == 0, b_ref[0:1, :], b_ref[1:2, :])
    rot = rot_ref[...]
    tile = 256
    ntile = n // tile
    full_rows = lambda c, p: pl.ds(pl.multiple_of(c * (2 * n) + p * n, n), n)

    def rope(v, p, r):
        ct = tab_v[p, pl.ds(r, tile), :HD]
        st = tab_v[p, pl.ds(r, tile), HD:]
        return (v.astype(f32) * ct + jnp.dot(v, rot, preferred_element_type=f32) * st).astype(bf16)

    def keys(p):
        def body(t, _):
            r = pl.multiple_of(t * tile, tile)
            h = hid_v[p, pl.ds(r, tile), :].astype(f32)
            inv = lax.rsqrt(jnp.mean(h * h, axis=-1, keepdims=True) + EPS_NORM)
            nv = (h * inv * gain).astype(bf16)
            nrm_v[pl.ds(p * n + r, tile), :] = nv
            kv = (jnp.dot(nv, w_v[:, aw:], preferred_element_type=f32) + bias[:, aw:]).astype(bf16)
            kv_v[pl.ds(p * n + r, tile), :kw] = rope(kv[:, :kw], p, r)
            kv_v[pl.ds(p * n + r, tile), kw:] = kv[:, kw:]
            return 0
        lax.fori_loop(0, ntile, body, 0)

    def queries(p):
        def body(t, _):
            r = pl.multiple_of(t * tile, tile)
            qv = (jnp.dot(nrm_v[pl.ds(p * n + r, tile), :], w_v[:, :aw], preferred_element_type=f32) + bias[:, :aw]).astype(bf16)
            for h in range(aw // HD):
                q_v[pl.ds(p * n + r, tile), h * HD:(h + 1) * HD] = rope(qv[:, h * HD:(h + 1) * HD], p, r)
            return 0
        lax.fori_loop(0, ntile, body, 0)

    def grads(p):
        def body(t, _):
            r = pl.multiple_of(t * tile, tile)
            gc_v[pl.ds(p * n + r, tile), :] = lax.dot_general(
                go_v[p, pl.ds(r, tile), :], wo_v[...], (((1,), (1,)), ((), ())), preferred_element_type=f32).astype(bf16)
            return 0
        lax.fori_loop(0, ntile, body, 0)

    def spread_kv(p):
        out = []
        for d, peer in enumerate((right, left)):
            c = pltpu.make_async_remote_copy(kv_v.at[p * n:(p + 1) * n, :], kv_all.at[full_rows(x, p), :],
                                             ksend.at[2 * p + d], krecv.at[2 * p + d], device_id={'x': peer}, device_id_type=MESH)
            c.start()
            out.append(c)
        return out

    for c in loads[:4]:
        c.wait()
    keys(0)
    sent = spread_kv(0)
    give[0].wait_recv()
    give[1].wait_recv()
    keys(1)
    sent += spread_kv(1)
    stores = [pltpu.make_async_copy(kv_v, kv_all.at[pl.ds(pl.multiple_of(x * (2 * n), 2 * n), 2 * n), :], loc.at[7]),
              pltpu.make_async_copy(nrm_v, normed, loc.at[8]),
              pltpu.make_async_copy(tab_v.at[0], tab2.at[0:n, :], loc.at[9]),
              pltpu.make_async_copy(tab_v.at[1], tab2.at[n:, :], loc.at[10])]
    for c in stores:
        c.start()
    loads[4].wait()
    queries(0)

    sent[0].wait_recv()
    on0 = pltpu.make_async_remote_copy(kv_all.at[full_rows(left, 0), :], kv_all.at[full_rows(left, 0), :],
                                       ksend.at[4], krecv.at[4], device_id={'x': right}, device_id_type=MESH)
    on0.start()
    queries(1)
    stores.append(pltpu.make_async_copy(q_v, q_out, loc.at[11]))
    stores[-1].start()
    sent[3].wait_recv()
    on1 = pltpu.make_async_remote_copy(kv_all.at[full_rows(right, 1), :], kv_all.at[full_rows(right, 1), :],
                                       ksend.at[5], krecv.at[5], device_id={'x': left}, device_id_type=MESH)
    on1.start()
    loads[5].wait()
    loads[6].wait()
    grads(0)
    give[2].wait_recv()
    stores.append(pltpu.make_async_copy(go_v.at[1], go_o, loc.at[12]))
    stores[-1].start()
    grads(1)
    stores.append(pltpu.make_async_copy(gc_v, gctx_out, loc.at[13]))
    stores[-1].start()
    for c in stores:
        c.wait()
    for c in give:
        c.wait_send()
    sent[1].wait_recv()
    sent[2].wait_recv()
    for c in sent:
        c.wait_send()
    on0.wait()
    on1.wait()


def front(hidden, grad_out, tab, norm_gain, bias, rot, w_qkv, w_out, nx, kw):
    n, d = hidden.shape
    att = w_out.shape[0]
    aw = att // CORES
    hbm = pl.BlockSpec(memory_space=pl.ANY)
    vmem = pl.BlockSpec(memory_space=pltpu.VMEM)
    sds = jax.ShapeDtypeStruct
    dma = pltpu.SemaphoreType.DMA
    return pl.pallas_call(
        functools.partial(front_kernel, n=n, nx=nx, aw=aw, kw=kw, att=att), name='front',
        in_specs=[hbm, hbm, hbm, vmem, vmem, vmem, hbm, hbm], out_specs=[hbm] * 6,
        out_shape=[sds((2 * n, d), bf16), sds((n, d), bf16), sds((2 * n, aw), bf16), sds((2 * n, aw), bf16),
                   sds((nx * 2 * n, 2 * kw), bf16), sds((2 * n, 2 * HD), f32)],
        scratch_shapes=[pltpu.VMEM((2, n, d), bf16), pltpu.VMEM((2, n, d), bf16), pltpu.VMEM((2, n, 2 * HD), f32),
                        pltpu.VMEM((2 * n, d), bf16), pltpu.VMEM((d, aw + 2 * kw), bf16), pltpu.VMEM((aw, d), bf16),
                        pltpu.VMEM((2 * n, aw), bf16), pltpu.VMEM((2 * n, aw), bf16), pltpu.VMEM((2 * n, 2 * kw), bf16),
                        dma((14,)), dma((3,)), dma((3,)), dma((6,)), dma((6,))],
        compiler_params=pltpu.CompilerParams(collective_id=0, has_side_effects=True, vmem_limit_bytes=60 << 20),
        cost_estimate=pl.CostEstimate(flops=60 * 10 ** 9, bytes_accessed=50 * 10 ** 6, transcendentals=0),
    )(hidden, grad_out, tab, norm_gain, bias, rot, w_qkv, w_out)


def block_table(qi, ds, swap, chip):
    q2, d2 = qi.reshape(-1, BQ), ds.reshape(-1, BQ)
    lo = d2[:, 0] // BK
    hi = q2[:, -1] // BK + 1
    flo = jnp.minimum((d2[:, -1] + BK - 1) // BK, hi)
    fhi = jnp.maximum((q2[:, 0] + 1) // BK, flo)
    return jnp.stack([lo, hi, flo, fhi, jnp.full_like(lo, swap), jnp.full_like(lo, chip)]).astype(jnp.int32)


def pair_swap():
    r = np.zeros((HD, HD), np.float32)
    for j in range(ROT_DIMS // 2):
        r[2 * j + 1, 2 * j] = -1.0
        r[2 * j, 2 * j + 1] = 1.0
    return r


def solution(mesh):
    axes = dict(mesh.shape)
    mesh3 = Mesh(mesh.devices.reshape(axes['dp'], axes['cp'] // CORES, CORES), ('dp', 'x', 'k'))
    flip = [(0, 1), (1, 0)]
    nx = mesh3.shape['x']

    def per_device(hidden, seg_id, doc_pos, norm_gain, w_qkv, b_qkv, w_out, grad_out):
        n, d = hidden.shape
        att = w_out.shape[0]
        kvw = (w_qkv.shape[1] - att) // 2
        aw, kw = att // CORES, kvw // CORES
        x, k = lax.axis_index('x'), lax.axis_index('k')
        other = lambda a: lax.ppermute(a, 'k', flip)
        both = lambda a: jnp.concatenate([a, other(a)], axis=0)
        ordered = lambda a, b: jnp.where(k == 0, jnp.concatenate([a, b], axis=1), jnp.concatenate([b, a], axis=1))

        pos2 = both(doc_pos)
        base = x * (CORES * n)
        qi = jnp.concatenate([base + k * n + jnp.arange(n), base + (1 - k) * n + jnp.arange(n)]).astype(jnp.int32)
        ds = qi - pos2
        meta = block_table(qi, ds, k, x)

        inv_freq = ROPE_BASE ** (-jnp.arange(0, ROT_DIMS, 2).astype(f32) / ROT_DIMS)
        ang = inv_freq[:, None] * doc_pos.astype(f32)[None, :]
        wide = lambda a, fill: jnp.concatenate([jnp.repeat(a, 2, axis=0), jnp.full((HD - ROT_DIMS, n), fill, f32)], axis=0)
        tab = jnp.concatenate([wide(jnp.cos(ang), 1.0), wide(jnp.sin(ang), 0.0)], axis=0).T
        bias = jnp.stack([jnp.concatenate([b_qkv[c * aw:(c + 1) * aw], b_qkv[att + c * kw:att + (c + 1) * kw],
                                           b_qkv[att + kvw + c * kw:att + kvw + (c + 1) * kw]]) for c in range(CORES)]).astype(f32)
        gain = norm_gain.astype(f32)
        normed, go_o, q, gctx, kv_all, tab2 = front(hidden, grad_out, tab, norm_gain[None], bias,
                                                     jnp.asarray(pair_swap(), bf16), w_qkv, w_out, nx, kw)
        ctx, lse, dd = flash_fwd(meta, q, gctx, kv_all, qi[None], ds[None], n)
        over = (((0,), (0,)), ((), ()))
        g_wout = (lax.dot_general(ctx[:n], grad_out, over, preferred_element_type=f32)
                  + lax.dot_general(ctx[n:], go_o, over, preferred_element_type=f32))
        lse, g_wout = lax.optimization_barrier((lse, g_wout))
        g_wout = lax.psum(g_wout, 'x')
        back = functools.partial(flash_bwd, meta, q, gctx, kv_all, qi[None], ds[None], lse, dd, n)
        dq_far, dkv = back()
        c_tok, s_tok = tab2[:, :HD], tab2[:, HD:]
        dkv, g_wout, dq_far = lax.optimization_barrier((dkv, g_wout, dq_far))
        dkv = lax.psum_scatter(dkv, 'x', scatter_dimension=0, tiled=True)
        dq, dkv_near = back(tab2, dq_far)
        dq, ctx = lax.optimization_barrier((dq, ctx))
        g_wq = lax.dot_general(normed, dq, over, preferred_element_type=f32)
        wout_o = other(g_wout)
        dq_all = ordered(dq[:n], other(dq[n:]))
        rows = (((1,), (1,)), ((), ()))
        gnorm = lax.dot_general(dq_all, w_qkv[:, :att], rows, preferred_element_type=f32)
        o_wout = jnp.where(k == 0, jnp.concatenate([g_wout, wout_o]), jnp.concatenate([wout_o, g_wout]))
        ctx_all = ordered(ctx[:n], other(ctx[n:]))
        y_out = (hidden.astype(f32) + jnp.dot(ctx_all, w_out, preferred_element_type=f32)).astype(bf16)
        g_wq, dkv = lax.optimization_barrier((g_wq, dkv))
        g_wq = lax.psum_scatter(g_wq, 'x', scatter_dimension=0, tiled=True)
        dkv = dkv + dkv_near
        dk = dkv[:, :kw] * SCALE
        dkt = jnp.dot(dk, jnp.asarray(pair_swap().T), precision=lax.Precision.HIGHEST, preferred_element_type=f32)
        gkv = jnp.concatenate([(dk * c_tok + dkt * s_tok).astype(bf16), dkv[:, kw:].astype(bf16)], axis=1)
        g_wkv = lax.dot_general(normed, gkv, over, preferred_element_type=f32)
        gkv_o = other(gkv[n:])
        gkv_all = jnp.concatenate([ordered(gkv[:n, :kw], gkv_o[:, :kw]), ordered(gkv[:n, kw:], gkv_o[:, kw:])], axis=1)
        gnorm = gnorm + lax.dot_general(gkv_all, w_qkv[:, att:], rows, preferred_element_type=f32)
        h32 = hidden.astype(f32)
        inv_rms = lax.rsqrt(jnp.mean(h32 * h32, axis=-1, keepdims=True) + EPS_NORM)
        x_hat = h32 * inv_rms
        scaled = gnorm * gain
        g_hidden = (grad_out.astype(f32) + inv_rms * (scaled - x_hat * jnp.mean(scaled * x_hat, axis=-1, keepdims=True))).astype(bf16)
        total = lambda a: jnp.sum(a.astype(f32), axis=0)
        sums = jnp.concatenate([total(gnorm * x_hat), total(dq_all), total(gkv_all)])
        srows = -(-sums.size // (2 * kw))
        sums = jnp.pad(sums, (0, srows * 2 * kw - sums.size)).reshape(srows, 2 * kw)
        g_wkv, g_wq, sums, g_hidden = lax.optimization_barrier((g_wkv, g_wq, sums, g_hidden))
        g_wkv = lax.psum_scatter(g_wkv, 'x', scatter_dimension=0, tiled=True)
        g_wq, g_wkv = lax.optimization_barrier((g_wq, g_wkv))
        by_chip = lambda g: lax.all_gather(g, ('x', 'k'), axis=0).reshape(nx, CORES, *g.shape)
        g_wq = by_chip(g_wq)
        g_wkv, g_wq, y_out, o_wout = lax.optimization_barrier((g_wkv, g_wq, y_out, o_wout))
        o_q = jnp.concatenate([g_wq[:, c] for c in range(CORES)], axis=-1).reshape(d, att)
        last = by_chip(jnp.concatenate([g_wkv, sums]))
        g_wkv = last[:, :, :d // nx]
        sums = jnp.sum(last[:, :, d // nx:], axis=(0, 1)).reshape(-1)
        o_kv = jnp.concatenate([g_wkv[:, c, :, p * kw:(p + 1) * kw] for p in range(2) for c in range(CORES)], axis=-1)
        o_wqkv = lax.dynamic_update_slice(jnp.pad(o_q, ((0, 0), (0, 2 * kvw))), o_kv.reshape(d, 2 * kvw), (0, att))
        return y_out, g_hidden, sums[:d], o_wqkv, sums[d:d + b_qkv.size], o_wout

    act = P(('dp', 'x', 'k'), None)
    row = P(('dp', 'x', 'k'))
    return jax.shard_map(per_device, mesh=mesh3,
                         in_specs=(act, row, row, P(), P(), P(), P(), act),
                         out_specs=(act, act, P('dp'), P('dp', None), P('dp'), P('dp', None)),
                         check_vma=False)
```
